32 devices in a mesh: row: 4 (over y, x), col: 8 (over z, core).
Axes of the slice: x: 2, y: 2, z: 4, core: 2. Of those that a mesh axis runs over, the one named last changes fastest.
Arguments:
- pair_act: float32 [768, 768, 128], P('row', 'col'), may hold values from -6 to 6
- grad_out: float32 [768, 768, 128], P('row', 'col'), may hold values from -6 to 6
- residue_mask: int32 [768], replicated, may hold values from 0 to 1, as said below
- norm_gains: float32 [2, 128], replicated, may hold values from 0.25 to 1.75
- weights: float32 [6, 128, 128], replicated, may hold values from -0.5 to 0.5
Outputs:
- grad_pair: float32 [768, 768, 128], P('row', 'col')
- grad_weights: float32 [6, 128, 128], replicated
- grad_gains: float32 [2, 128], replicated
The draws below stay inside these ranges and needn't reach their ends.
Inputs may be any that keep to these rules, and one draw needn't show every extreme that they name: `residue_mask`: the residues form four stretches of 192; in each stretch the valid residues are a prefix of at least 96 and fewer than 192 residues.
All inputs are finite; a program needn't handle non-finite values.
Results may differ from the reference program's by a relative error of at most 0.00009.
Values sent between devices are 32-bit elements; how exact they have to be, the bound alone decides.
No kernel may reach another device: no remote copies, remote signals or barrier semaphores. Data moves between devices by JAX's collectives and lax.ppermute only.
A program may use at most 320 MiB of HBM per device.

```python
import jax
import jax.numpy as jnp
from jax import lax

C = 128
N = 768


def draw_residue_mask(key, part):
    stretch = N // 4
    subkeys = jax.random.split(jax.random.fold_in(key, 17), 1)
    lengths = jax.random.randint(subkeys[0], (4,), stretch // 2, stretch)
    position = jnp.arange(N) % stretch
    stretch_id = jnp.arange(N) // stretch
    return (position < lengths[stretch_id]).astype(jnp.int32)


def shard_levels(key, shape, cuts, low, largest):
    factor_of = 1.0
    for dim, shards_of in cuts:
        draws = jax.random.uniform(jax.random.fold_in(jax.random.fold_in(key, 6), dim), (shards_of,), jnp.float32, low / len(cuts), largest / len(cuts))
        factor_of = factor_of * jnp.repeat(jnp.exp(draws), shape[dim] // shards_of).reshape((-1,) + (1,) * (len(shape) - 1 - dim))
    return factor_of


def normal_values(stream_key, dims, width, reach, shards=(), dtype=jnp.bfloat16):
    drawn = width * jax.random.normal(stream_key, dims, jnp.float32)
    if shards:
        drawn = drawn * shard_levels(stream_key, dims, shards, -0.22, 0.18)
    return jnp.clip(drawn, -reach, reach).astype(dtype)


def setup_inputs(seed: int = 0) -> dict:
    key_list = jax.random.split(jax.random.key(seed), 6)
    pair_act = normal_values(key_list[0], (N, N, C), 1.0, 6.0, ((0, 4), (1, 8)), jnp.float32)
    grad_out = normal_values(key_list[1], (N, N, C), 1.0, 6.0, ((0, 4), (1, 8)), jnp.float32)
    residue_mask = draw_residue_mask(jax.random.fold_in(key_list[5], 71), 0)
    norm_gains = jnp.clip(1.0 + 0.15 * jax.random.normal(key_list[3], (2, C), jnp.float32), 0.25, 1.75)
    weights = normal_values(key_list[4], (6, C, C), C ** -0.5, 0.5, (), jnp.float32)
    return {"pair_act": pair_act, "grad_out": grad_out, "residue_mask": residue_mask, "norm_gains": norm_gains, "weights": weights}


epsilon = 1e-05
block_rows = 32
highest = lax.Precision.HIGHEST

def norm_parts(operand):
    average = lax.optimization_barrier(jnp.mean(operand, axis=-1, keepdims=True))
    centered = operand - average
    inv_std = lax.rsqrt(lax.optimization_barrier(jnp.mean(centered * centered, axis=-1, keepdims=True)) + epsilon)
    return (centered * inv_std, inv_std)

def norm_back(grad_hat, normed, inv_std):
    first_mean = lax.optimization_barrier(jnp.mean(grad_hat, axis=-1, keepdims=True))
    second_mean = lax.optimization_barrier(jnp.mean(grad_hat * normed, axis=-1, keepdims=True))
    return inv_std * (grad_hat - first_mean - normed * second_mean)

def project(operand, weight):
    return jnp.einsum('ijc,cd->ijd', operand, weight, precision=highest)

def sigmoid(operand):
    return 1.0 / (1.0 + jnp.exp(-operand))

def input_side(pair_rows, mask_rows, residue_mask, norm_gains, weights):
    pair_hat, inv_std = norm_parts(pair_rows)
    normed = pair_hat * norm_gains[0]
    pair_mask = (mask_rows[:, None] * residue_mask[None, :]).astype(jnp.float32)[:, :, None]
    lin_a = project(normed, weights[0])
    sig_a = sigmoid(project(normed, weights[1]))
    lin_b = project(normed, weights[2])
    sig_b = sigmoid(project(normed, weights[3]))
    return (pair_hat, inv_std, normed, pair_mask, lin_a, sig_a, lin_b, sig_b)

def output_side(normed, tri_rows, grad_rows, norm_gains, weights):
    tri_hat, tri_inv = norm_parts(tri_rows)
    tri_norm = tri_hat * norm_gains[1]
    lin_o = project(tri_norm, weights[5])
    sig_g = sigmoid(project(normed, weights[4]))
    d_out = grad_rows * sig_g
    d_gate = grad_rows * lin_o * sig_g * (1.0 - sig_g)
    d_norm = project(d_out, weights[5].T)
    d_tri = norm_back(d_norm * norm_gains[1], tri_hat, tri_inv)
    return (tri_hat, tri_norm, d_out, d_gate, d_norm, d_tri)

def reference(pair_act, grad_out, residue_mask, norm_gains, weights):
    residues = pair_act.shape[0]
    channels = pair_act.shape[2]
    blocks = residues // block_rows
    full_shape = pair_act.shape
    block_shape = (blocks, block_rows, residues, channels)
    mask_blocks = residue_mask.reshape(blocks, block_rows)

    def first_pass(inputs_block):
        pair_rows, mask_rows = inputs_block
        sides = input_side(pair_rows, mask_rows, residue_mask, norm_gains, weights)
        pair_mask = sides[3]
        return (pair_mask * sides[5] * sides[4], pair_mask * sides[7] * sides[6])
    act_a, act_b = lax.map(first_pass, (pair_act.reshape(block_shape), mask_blocks))
    act_a = act_a.reshape(full_shape)
    act_b = act_b.reshape(full_shape)
    triangle = jnp.einsum('ikc,jkc->ijc', act_a, act_b, precision=highest)

    def second_pass(inputs_block):
        pair_rows, tri_rows, grad_rows = inputs_block
        pair_hat, inv_std = norm_parts(pair_rows)
        normed = pair_hat * norm_gains[0]
        outside = output_side(normed, tri_rows, grad_rows, norm_gains, weights)
        tri_hat, tri_norm, d_out, d_norm, d_tri = (outside[0], outside[1], outside[2], outside[4], outside[5])
        grad_o = jnp.einsum('ijc,ijd->cd', tri_norm, d_out, precision=highest)
        gain_two = lax.optimization_barrier(jnp.sum(d_norm * tri_hat, axis=(0, 1)))
        return (d_tri, grad_o, gain_two)
    d_tri, grad_o, gain_two = lax.map(second_pass, (pair_act.reshape(block_shape), triangle.reshape(block_shape), grad_out.reshape(block_shape)))
    d_tri = d_tri.reshape(full_shape)
    grad_o = lax.optimization_barrier(jnp.sum(grad_o, axis=0))
    gain_two = lax.optimization_barrier(jnp.sum(gain_two, axis=0))
    d_act_a = jnp.einsum('ijc,jkc->ikc', d_tri, act_b, precision=highest)
    d_act_b = jnp.einsum('ijc,ikc->jkc', d_tri, act_a, precision=highest)

    def third_pass(inputs_block):
        pair_rows, mask_rows, tri_rows, grad_rows, da_rows, db_rows = inputs_block
        pair_hat, inv_std, normed, pair_mask, lin_a, sig_a, lin_b, sig_b = input_side(pair_rows, mask_rows, residue_mask, norm_gains, weights)
        d_gate = output_side(normed, tri_rows, grad_rows, norm_gains, weights)[3]
        d_lin_a = da_rows * pair_mask * sig_a
        d_sig_a = da_rows * pair_mask * lin_a * sig_a * (1.0 - sig_a)
        d_lin_b = db_rows * pair_mask * sig_b
        d_sig_b = db_rows * pair_mask * lin_b * sig_b * (1.0 - sig_b)
        d_normed = project(d_lin_a, weights[0].T) + project(d_sig_a, weights[1].T)
        d_normed = d_normed + project(d_lin_b, weights[2].T) + project(d_sig_b, weights[3].T)
        d_normed = d_normed + project(d_gate, weights[4].T)
        weight_grads = jnp.stack([jnp.einsum('ijc,ijd->cd', normed, d_lin_a, precision=highest), jnp.einsum('ijc,ijd->cd', normed, d_sig_a, precision=highest), jnp.einsum('ijc,ijd->cd', normed, d_lin_b, precision=highest), jnp.einsum('ijc,ijd->cd', normed, d_sig_b, precision=highest), jnp.einsum('ijc,ijd->cd', normed, d_gate, precision=highest)])
        gain_one = lax.optimization_barrier(jnp.sum(d_normed * pair_hat, axis=(0, 1)))
        grad_rows_pair = norm_back(d_normed * norm_gains[0], pair_hat, inv_std)
        return (grad_rows_pair, weight_grads, gain_one)
    grad_pair, weight_grads, gain_one = lax.map(third_pass, (pair_act.reshape(block_shape), mask_blocks, triangle.reshape(block_shape), grad_out.reshape(block_shape), d_act_a.reshape(block_shape), d_act_b.reshape(block_shape)))
    grad_pair = grad_pair.reshape(full_shape)
    weight_grads = lax.optimization_barrier(jnp.sum(weight_grads, axis=0))
    gain_one = lax.optimization_barrier(jnp.sum(gain_one, axis=0))
    grad_weights = jnp.concatenate([weight_grads, grad_o[None]], axis=0) / residues
    grad_gains = jnp.stack([gain_one, gain_two]) / residues
    return (grad_pair, grad_weights, grad_gains)
```

```python
import jax
import jax.numpy as jnp
from jax import lax
from jax.sharding import PartitionSpec as P

epsilon = 1e-05
highest = lax.Precision.HIGH


def norm_parts(operand):
    average = jnp.mean(operand, axis=-1, keepdims=True)
    centered = operand - average
    inv_std = lax.rsqrt(jnp.mean(centered * centered, axis=-1, keepdims=True) + epsilon)
    return (centered * inv_std, inv_std)


def norm_back(grad_hat, normed, inv_std):
    first_mean = jnp.mean(grad_hat, axis=-1, keepdims=True)
    second_mean = jnp.mean(grad_hat * normed, axis=-1, keepdims=True)
    return inv_std * (grad_hat - first_mean - normed * second_mean)


def project(operand, weight):
    return jnp.einsum("ijc,cd->ijd", operand, weight, precision=highest)


def sigmoid(operand):
    return 1.0 / (1.0 + jnp.exp(-operand))


def chunk_count(channels):
    local_chans = channels // (lax.axis_size("row") * lax.axis_size("col"))
    return 2 if local_chans % 2 == 0 else 1


def exchange(blocks):
    return lax.all_to_all(blocks, ("row", "col"), split_axis=0, concat_axis=0, tiled=True)


def to_channels(tiles):
    tile_rows, tile_cols, channels = tiles.shape
    row_count = lax.axis_size("row")
    col_count = lax.axis_size("col")
    pieces = chunk_count(channels)
    blocks = jnp.transpose(tiles, (2, 0, 1)).reshape(
        row_count * col_count, pieces, -1, tile_rows, tile_cols
    )
    result = []
    for piece in range(pieces):
        arrived = exchange(blocks[:, piece])
        shaped = arrived.reshape(row_count, col_count, -1, tile_rows, tile_cols)
        shaped = jnp.transpose(shaped, (2, 0, 3, 1, 4))
        result.append(shaped.reshape(-1, row_count * tile_rows, col_count * tile_cols))
    return result


def send_back(chans, tile_rows, tile_cols):
    row_count = lax.axis_size("row")
    col_count = lax.axis_size("col")
    shaped = chans.reshape(-1, row_count, tile_rows, col_count, tile_cols)
    shaped = jnp.transpose(shaped, (1, 3, 0, 2, 4))
    return exchange(shaped.reshape(row_count * col_count, -1, tile_rows, tile_cols))


def to_positions(arrived):
    tile_rows, tile_cols = arrived[0].shape[2:]
    joined = jnp.stack(arrived, axis=1).reshape(-1, tile_rows, tile_cols)
    return jnp.transpose(joined, (1, 2, 0))


def on_device(pair_act, grad_out, residue_mask, norm_gains, weights):
    tile_rows, tile_cols, channels = pair_act.shape
    residues = residue_mask.shape[0]
    row_mask = lax.dynamic_slice_in_dim(residue_mask, lax.axis_index("row") * tile_rows, tile_rows)
    col_mask = lax.dynamic_slice_in_dim(residue_mask, lax.axis_index("col") * tile_cols, tile_cols)
    pair_mask = (row_mask[:, None] * col_mask[None, :]).astype(jnp.float32)[:, :, None]
    pair_hat, inv_std = norm_parts(pair_act)
    normed = pair_hat * norm_gains[0]
    lin_a = project(normed, weights[0])
    sig_a = sigmoid(project(normed, weights[1]))
    lin_b = project(normed, weights[2])
    sig_b = sigmoid(project(normed, weights[3]))
    chan_a = to_channels(pair_mask * sig_a * lin_a)
    chan_b = to_channels(pair_mask * sig_b * lin_b)
    tri_parts = []
    for left, right in zip(chan_a, chan_b):
        chan_tri = jnp.einsum("lik,ljk->lij", left, right, precision=highest)
        tri_parts.append(send_back(chan_tri, tile_rows, tile_cols))
    triangle = to_positions(tri_parts)
    tri_hat, tri_inv = norm_parts(triangle)
    tri_norm = tri_hat * norm_gains[1]
    lin_o = project(tri_norm, weights[5])
    sig_g = sigmoid(project(normed, weights[4]))
    d_out = grad_out * sig_g
    d_gate = grad_out * lin_o * sig_g * (1.0 - sig_g)
    d_norm = project(d_out, weights[5].T)
    d_tri = norm_back(d_norm * norm_gains[1], tri_hat, tri_inv)
    da_parts = []
    db_parts = []
    for left, right, chan_dtri in zip(chan_a, chan_b, to_channels(d_tri)):
        chan_da = jnp.einsum("lij,ljk->lik", chan_dtri, right, precision=highest)
        da_parts.append(send_back(chan_da, tile_rows, tile_cols))
        chan_db = jnp.einsum("lij,lik->ljk", chan_dtri, left, precision=highest)
        db_parts.append(send_back(chan_db, tile_rows, tile_cols))
    d_acts = [to_positions(da_parts), to_positions(db_parts)]
    d_lin_a = d_acts[0] * pair_mask * sig_a
    d_sig_a = d_acts[0] * pair_mask * lin_a * sig_a * (1.0 - sig_a)
    d_lin_b = d_acts[1] * pair_mask * sig_b
    d_sig_b = d_acts[1] * pair_mask * lin_b * sig_b * (1.0 - sig_b)
    grads_cat = jnp.concatenate([d_lin_a, d_sig_a, d_lin_b, d_sig_b, d_gate], axis=-1).reshape(
        -1, 5 * channels
    )
    weights_turned = jnp.transpose(weights[:5], (0, 2, 1)).reshape(5 * channels, channels)
    d_normed = jnp.dot(grads_cat, weights_turned, precision=highest).reshape(
        tile_rows, tile_cols, channels
    )
    flat_normed = normed.reshape(-1, channels)
    weight_part = jnp.einsum("pc,pd->cd", flat_normed, grads_cat, precision=highest)
    weight_part = jnp.transpose(weight_part.reshape(channels, 5, channels), (1, 0, 2)).reshape(
        5 * channels, channels
    )
    out_part = jnp.einsum(
        "pc,pd->cd", tri_norm.reshape(-1, channels), d_out.reshape(-1, channels), precision=highest
    )
    gain_one = jnp.sum(d_normed * pair_hat, axis=(0, 1))
    gain_two = jnp.sum(d_norm * tri_hat, axis=(0, 1))
    grad_pair = norm_back(d_normed * norm_gains[0], pair_hat, inv_std)
    combined = jnp.concatenate([weight_part, out_part, gain_one[None], gain_two[None]], axis=0)
    column_total = lax.psum(combined, "col")
    total = lax.psum(column_total, "row")
    scaled = total / residues
    grad_weights = scaled[: 6 * channels].reshape(6, channels, channels)
    grad_gains = scaled[6 * channels :]
    return (grad_pair, grad_weights, grad_gains)


def solution(mesh):
    return jax.shard_map(
        on_device,
        mesh=mesh,
        in_specs=(P("row", "col", None), P("row", "col", None), P(), P(), P()),
        out_specs=(P("row", "col", None), P(), P()),
        check_vma=False,
    )
```
